32 devices in a mesh: row: 8 (over y, x, core), col: 4 (over z).
Axes of the slice: x: 2, y: 2, z: 4, core: 2. Of those that a mesh axis runs over, the one named last changes fastest.
Arguments:
- trailing: bfloat16 [4096, 8192], P('row', 'col'), may hold values from -6 to 6
- col_u: bfloat16 [8, 512, 64], P('row', 'col'), may hold values from -6 to 6
- col_v: bfloat16 [8, 512, 64], P('row', 'col'), may hold values from -0.75 to 0.75
- row_u: bfloat16 [16, 512, 64], P('col', 'row'), may hold values from -6 to 6
- row_v: bfloat16 [16, 512, 64], P('col', 'row'), may hold values from -0.03125 to 0.03125
- diag_lower_inv: float32 [512, 512], replicated, may hold values from -0.176776695 to 1, as said below
- diag_upper_inv: float32 [512, 512], replicated, may hold values from -0.176776695 to 2, as said below
Outputs:
- schur: bfloat16 [4096, 8192], P('row', 'col')
The draws below stay inside these ranges and needn't reach their ends.
Inputs may be any that keep to these rules, and one draw needn't show every extreme that they name: `diag_lower_inv`: lower triangular with unit diagonal. `diag_upper_inv`: upper triangular with diagonal entries between 0.5 and 2.
All inputs are finite; a program needn't handle non-finite values.
Results may differ from the reference program's by a relative error of at most 0.0054.
Values may be sent and summed in bfloat16 or wider, within the bound.
A program may use at most 64 MiB of HBM per device.

```python
import jax
import jax.numpy as jnp
from jax import lax

B = 512
R = 64
MT = 8
NT = 16


def draw_diag_lower_inv(key, part):
    noise = jnp.clip(jax.random.normal(jax.random.fold_in(key, 11), (B, B), jnp.float32), -4.0, 4.0)
    below = jnp.tril(noise, -1) / jnp.sqrt(jnp.float32(B))
    return below + jnp.eye(B, dtype=jnp.float32)


def draw_diag_upper_inv(key, part):
    noise = jnp.clip(jax.random.normal(jax.random.fold_in(key, 23), (B, B), jnp.float32), -4.0, 4.0)
    above = jnp.triu(noise, 1) / jnp.sqrt(jnp.float32(B))
    pivots = jax.random.uniform(jax.random.fold_in(key, 37), (B,), jnp.float32, 0.5, 2.0)
    return above + jnp.diag(pivots)


def level_of(own_key, dims, shards, low, top_value):
    def one(axis_at, blocks):
        steps = jax.random.uniform(jax.random.fold_in(jax.random.fold_in(own_key, 6), axis_at), (blocks,), jnp.float32, low / len(shards), top_value / len(shards))
        return jnp.repeat(jnp.exp(steps), dims[axis_at] // blocks).reshape((-1,) + (1,) * (len(dims) - axis_at - 1))

    gain = one(*shards[0])
    for cut in shards[1:]:
        gain = gain * one(*cut)
    return gain


def normal_values(own_key, dims, scale, limit, pieces=(), kind=jnp.bfloat16):
    values = scale * jax.random.normal(own_key, dims, jnp.float32)
    if pieces:
        values = values * level_of(own_key, dims, pieces, -0.22, 0.18)
    return jnp.clip(values, -limit, limit).astype(kind)


def setup_inputs(seed: int = 0) -> dict:
    key_of = jax.random.split(jax.random.key(seed), 8)
    trailing = normal_values(key_of[0], (MT * B, NT * B), 1.0, 6.0, ((0, 8), (1, 4)))
    col_u = normal_values(key_of[1], (MT, B, R), 1.0, 6.0, ((0, 8), (1, 4)))
    col_v = normal_values(key_of[2], (MT, B, R), R ** -0.5, 0.75, ((0, 8), (1, 4)))
    row_u = normal_values(key_of[3], (NT, B, R), 1.0, 6.0, ((0, 4), (1, 8)))
    row_v = normal_values(key_of[4], (NT, B, R), (R * B) ** -0.5, 0.03125, ((0, 4), (1, 8)))
    diag_lower_inv = draw_diag_lower_inv(jax.random.fold_in(key_of[7], 71), 0)
    diag_upper_inv = draw_diag_upper_inv(jax.random.fold_in(key_of[7], 71), 0)
    return {"trailing": trailing, "col_u": col_u, "col_v": col_v, "row_u": row_u, "row_v": row_v, "diag_lower_inv": diag_lower_inv, "diag_upper_inv": diag_upper_inv}


def reference(trailing, col_u, col_v, row_u, row_v, diag_lower_inv, diag_upper_inv):
    highest = lax.Precision.HIGHEST
    left_v = jnp.einsum("ba,tbr->tar", diag_upper_inv, col_v.astype(jnp.float32), precision=highest)
    lower = jnp.einsum("tpr,tar->tpa", col_u.astype(jnp.float32), left_v, precision=highest).astype(jnp.bfloat16)
    right_u = jnp.einsum("ab,tbr->tar", diag_lower_inv, row_u.astype(jnp.float32), precision=highest)
    upper = jnp.einsum("tar,tqr->taq", right_u, row_v.astype(jnp.float32), precision=highest).astype(jnp.bfloat16)
    upper_whole = jnp.transpose(upper, (1, 0, 2)).reshape(B, NT * B)

    def update(pair):
        rows, tile = pair
        product = jnp.dot(tile, upper_whole, preferred_element_type=jnp.float32)
        return (rows.astype(jnp.float32) - product).astype(jnp.bfloat16)

    blocks = lax.map(update, (trailing.reshape(MT, B, NT * B), lower))
    return blocks.reshape(MT * B, NT * B)
```

```python
import functools

import jax
import jax.numpy as jnp
from jax import lax
from jax.experimental import pallas as pl
from jax.experimental.pallas import tpu as pltpu
from jax.sharding import PartitionSpec as P

MESH = pl.DeviceIdType.MESH
F32 = jnp.float32
BF16 = jnp.bfloat16
BLOCKS = 1


def partner(at, step, count):
    if count & (count - 1):
        return lax.rem(at + step, count)
    out = jnp.int32(0)
    weight = 1
    while weight < count:
        bit = (at // weight) % 2
        out = out + weight * ((1 - bit) if step & weight else bit)
        weight *= 2
    return out


def source(at, step, count):
    if count & (count - 1):
        return lax.rem(at + count - step, count)
    return partner(at, step, count)


def split(x):
    high = x.astype(BF16)
    return high, (x - high.astype(F32)).astype(BF16)


def dot(a, b):
    return lax.dot_general(a, b, (((1,), (0,)), ((), ())), preferred_element_type=F32)


def dot_rt(a, b):
    return lax.dot_general(a, b, (((1,), (1,)), ((), ())), preferred_element_type=F32)


def pack(left, right):
    return jnp.concatenate([left.astype(F32), right.astype(F32)], axis=-1).astype(BF16)


def panel_kernel(
    n_row, n_col,
    cu_hbm, cv_hbm, ru_hbm, rv_hbm, dl_hbm, du_hbm, trail_hbm,
    t_ref, cu_ref, trail,
    ru, rv, dl, du, mh, ml, cuall, cvall, gall,
    in_sem, cu_send, cu_recv, cv_send, cv_recv, row_send, row_recv, fwd_send, row_hello, col_hello,
):
    row = lax.axis_index("row")
    col = lax.axis_index("col")
    paired = n_row % 2 == 0
    width = 2 if paired else 1
    chips = n_row // width
    core = row % width
    chip = row // width

    col_steps = list(range(n_col - 1, 0, -1))
    chip_steps = list(range(chips - 1, 0, -1))
    col_to = {k: partner(col, k, n_col) for k in col_steps}
    col_from = {k: source(col, k, n_col) for k in col_steps}
    row_to = {k: partner(chip, k, chips) * width + core for k in chip_steps}
    row_from = {k: source(chip, k, chips) * width + core for k in chip_steps}
    mate = chip * width + (1 - core) if paired else row

    col_peers = [col_to[k] for k in col_steps]
    chip_peers = [row_to[k] for k in chip_steps]
    if paired:
        chip_peers.append(mate)

    barrier = pltpu.get_barrier_semaphore()
    for to in chip_peers:
        @pl.when(to > row)
        def _():
            pl.semaphore_signal(barrier, inc=1, device_id=(to, col), device_id_type=MESH)
    for to in col_peers:
        @pl.when(to > col)
        def _():
            pl.semaphore_signal(barrier, inc=1, device_id=(row, to), device_id_type=MESH)

    loads = []
    for n, (src, dst) in enumerate([
        (ru_hbm, ru), (rv_hbm, rv), (cv_hbm, cvall.at[col]), (cu_hbm, cuall.at[col]),
        (dl_hbm, dl), (du_hbm, du), (trail_hbm, trail),
    ]):
        load = pltpu.make_async_copy(src, dst, in_sem.at[n])
        load.start()
        loads.append(load)

    lower = chip + (core if paired else 0) + col

    @pl.when(lower > 0)
    def _():
        pl.semaphore_wait(barrier, lower)

    for to in chip_peers:
        @pl.when(to < row)
        def _():
            pl.semaphore_signal(row_hello.at[row], inc=1, device_id=(to, col), device_id_type=MESH)
    for to in col_peers:
        @pl.when(to < col)
        def _():
            pl.semaphore_signal(col_hello.at[col], inc=1, device_id=(row, to), device_id_type=MESH)

    loads[0].wait()
    loads[1].wait()
    gall[row] = pack(ru[...], rv[...])
    loads[2].wait()
    loads[3].wait()

    def row_copy(slot, send_sem, to):
        return pltpu.make_async_remote_copy(
            src_ref=gall.at[slot], dst_ref=gall.at[slot], send_sem=send_sem,
            recv_sem=row_recv.at[slot], device_id=(to, col), device_id_type=MESH,
        )

    def col_copy(slots, recv, slot, send_sem, to):
        return pltpu.make_async_remote_copy(
            src_ref=slots.at[slot], dst_ref=slots.at[slot], send_sem=send_sem,
            recv_sem=recv.at[slot], device_id=(row, to), device_id_type=MESH,
        )

    row_sends = [(row_to[k], row_copy(row, row_send.at[k], row_to[k])) for k in chip_steps]
    if paired:
        row_sends.append((mate, row_copy(row, row_send.at[0], mate)))
    col_sends = [
        (col_to[k], col_copy(slots, recv, col, send.at[k], col_to[k]))
        for slots, recv, send in ((cvall, cv_recv, cv_send), (cuall, cu_recv, cu_send))
        for k in col_steps
    ]
    for to, copy in col_sends:
        pl.when(to < col)(copy.start)
    for to, copy in row_sends:
        pl.when(to < row)(copy.start)
    sends = [copy for _, copy in row_sends + col_sends]

    loads[4].wait()
    loads[5].wait()
    order = dl.shape[0]
    half = order // 2
    uh, ul = split(du[...])
    lh, ll = split(dl[...])

    def product(rows, mid, cols):
        a, b = uh[rows, mid], ul[rows, mid]
        c, d = lh[mid, cols], ll[mid, cols]
        return dot(a, c) + (dot(a, d) + dot(b, c))

    lo, hi, full = slice(0, half), slice(half, order), slice(0, order)
    for rows, mid, cols in ((lo, full, lo), (lo, hi, hi), (hi, hi, lo), (hi, hi, hi)):
        mh[rows, cols], ml[rows, cols] = split(product(rows, mid, cols))

    for to, copy in reversed(row_sends):
        @pl.when(to > row)
        def _():
            pl.semaphore_wait(row_hello.at[to], 1)
            copy.start()
    for k in reversed(col_steps):
        to = col_to[k]

        @pl.when(to > col)
        def _():
            pl.semaphore_wait(col_hello.at[to], 1)
            col_copy(cvall, cv_recv, col, cv_send.at[k], to).start()
            col_copy(cuall, cu_recv, col, cu_send.at[k], to).start()

    for k in reversed(chip_steps):
        slot = row_from[k]
        row_copy(slot, row_send.at[k], row_to[k]).wait_recv()
        if paired:
            sends.append(row_copy(slot, fwd_send.at[k], mate))
            sends[-1].start()

    tiles, rank = cvall.shape[1], cvall.shape[2]
    for k in reversed(col_steps):
        col_copy(cvall, cv_recv, col_from[k], cv_send.at[k], col_to[k]).wait_recv()
    weights = []
    for t in range(tiles):
        turned = jnp.concatenate([cvall[c, t] for c in range(n_col)], axis=-1)
        wh, wl = split(dot(turned, mh[...]) + dot(turned, ml[...]))
        weights.append(jnp.concatenate([wh, wl], axis=0))

    for k in reversed(col_steps):
        col_copy(cuall, cu_recv, col_from[k], cu_send.at[k], col_to[k]).wait_recv()
    lefts = []
    for t in range(tiles):
        turned = jnp.concatenate([cuall[c, t] for c in range(n_col)], axis=-1).astype(F32)
        lefts.append(jnp.concatenate([turned, turned], axis=0).T.astype(BF16))

    if paired:
        row_copy(mate, row_send.at[0], mate).wait_recv()
        for k in reversed(chip_steps):
            slot = source(chip, k, chips) * width + (1 - core)
            row_copy(slot, fwd_send.at[k], mate).wait_recv()
    loads[6].wait()

    panels = [gall[:, j].reshape(order, 2 * rank) for j in range(gall.shape[1])]
    spread = jnp.concatenate(panels, axis=-1)
    for t in range(tiles):
        c = dot(weights[t], spread)
        c = c[:rank] + c[rank:]
        rights = []
        for j, g in enumerate(panels):
            core_j = c[:, 2 * rank * j:2 * rank * j + rank]
            ch, cl = split(jnp.concatenate([jnp.zeros_like(core_j), core_j], axis=-1))
            right = dot_rt(jnp.concatenate([ch, cl], axis=0), g)
            th, tl = split(right[:rank] + right[rank:])
            rights.append(jnp.concatenate([th, tl], axis=0))
        cu_ref[t] = lefts[t]
        for j, right in enumerate(rights):
            t_ref[t, :, pl.ds(j * order, order)] = right

    for send in sends:
        send.wait_send()


def update_kernel(blocks, t_ref, cu_ref, trail, out_hbm, out, out_sem):
    tiles, order, _ = cu_ref.shape
    wide = t_ref.shape[2] // blocks
    copies = []
    for t in range(tiles):
        rows = pl.ds(t * order, order)
        for b in range(blocks):
            at = pl.ds(b * wide, wide)
            product = dot(cu_ref[t], t_ref[t, :, at])
            out[rows, at] = (trail[rows, at].astype(F32) - product).astype(BF16)
            copy = pltpu.make_async_copy(out.at[rows, at], out_hbm.at[rows, at], out_sem.at[t * blocks + b])
            copy.start()
            copies.append(copy)
    for copy in copies:
        copy.wait()


def shards(n_row, n_col, trailing, col_u, col_v, row_u, row_v, diag_lower_inv, diag_upper_inv):
    mt, cc, rank = col_u.shape
    nt, rc, _ = row_u.shape
    order = diag_lower_inv.shape[0]
    anywhere = pl.BlockSpec(memory_space=pl.ANY)
    dma = pltpu.SemaphoreType.DMA
    wide = nt * order
    vmem = pl.BlockSpec(memory_space=pltpu.VMEM)
    handed = pl.pallas_call(
        functools.partial(panel_kernel, n_row, n_col),
        out_shape=[
            pltpu.VMEM((mt, 2 * rank, wide), BF16),
            pltpu.VMEM((mt, order, 2 * rank), BF16),
            pltpu.VMEM(trailing.shape, BF16),
        ],
        in_specs=[anywhere] * 7,
        out_specs=[vmem] * 3,
        scratch_shapes=[
            pltpu.VMEM(row_u.shape, BF16),
            pltpu.VMEM(row_v.shape, BF16),
            pltpu.VMEM((order, order), F32),
            pltpu.VMEM((order, order), F32),
            pltpu.VMEM((order, order), BF16),
            pltpu.VMEM((order, order), BF16),
            pltpu.VMEM((n_col, mt, rank, cc), BF16),
            pltpu.VMEM((n_col, mt, rank, cc), BF16),
            pltpu.VMEM((n_row, nt, rc, 2 * rank), BF16),
            dma((7,)), dma((n_col,)), dma((n_col,)), dma((n_col,)), dma((n_col,)),
            dma((n_row,)), dma((n_row,)), dma((n_row,)),
            pltpu.SemaphoreType.REGULAR((n_row,)), pltpu.SemaphoreType.REGULAR((n_col,)),
        ],
        compiler_params=pltpu.CompilerParams(collective_id=0, has_side_effects=True),
        name="panels",
    )(
        jnp.swapaxes(col_u, 1, 2), jnp.swapaxes(col_v, 1, 2), row_u, row_v,
        diag_lower_inv, diag_upper_inv, trailing,
    )
    handed = [pltpu.with_memory_space_constraint(x, pltpu.VMEM) for x in handed]
    blocks = BLOCKS * nt
    return pl.pallas_call(
        functools.partial(update_kernel, blocks),
        out_shape=jax.ShapeDtypeStruct(trailing.shape, BF16),
        in_specs=[vmem] * 3,
        out_specs=anywhere,
        scratch_shapes=[pltpu.VMEM(trailing.shape, BF16), dma((mt * blocks,))],
        name="update",
    )(*handed)


def solution(mesh):
    placed = (
        P("row", "col"),
        P("row", "col", None),
        P("row", "col", None),
        P("col", "row", None),
        P("col", "row", None),
        P(),
        P(),
    )
    return jax.shard_map(
        functools.partial(shards, mesh.shape["row"], mesh.shape["col"]),
        mesh=mesh, in_specs=placed, out_specs=P("row", "col"), check_vma=False,
    )
```

```python
import functools

import jax
import jax.numpy as jnp
from jax import lax
from jax.experimental import pallas as pl
from jax.experimental.pallas import tpu as pltpu
from jax.sharding import PartitionSpec as P

MESH = pl.DeviceIdType.MESH
F32 = jnp.float32
BF16 = jnp.bfloat16
LANES = 128
BLOCKS = 1


def others(at, count):
    if count & (count - 1):
        return [(step, lax.rem(at + step, count), count - step) for step in range(1, count)]
    out = []
    for step in range(1, count):
        to, weight = jnp.int32(0), 1
        while weight < count:
            bit = (at // weight) % 2
            to = to + weight * ((1 - bit) if step & weight else bit)
            weight *= 2
        out.append((step, to, step))
    return out


def split(x):
    high = x.astype(BF16)
    return high, (x - high.astype(F32)).astype(BF16)


def dot(a, b):
    return lax.dot_general(a, b, (((1,), (0,)), ((), ())), preferred_element_type=F32)


def dot_rt(a, b):
    return lax.dot_general(a, b, (((1,), (1,)), ((), ())), preferred_element_type=F32)


def pack(x, width):
    if width == 1:
        return x
    x = x.astype(F32)
    return jnp.stack([
        jnp.concatenate([x[p * width + w] for w in range(width)], axis=-1)
        for p in range(x.shape[0] // width)
    ]).astype(BF16)


def panel_kernel(
    n_row, n_col, order, rank,
    cu_hbm, cv_hbm, ru_hbm, rv_hbm, dl_hbm, du_hbm, trail_hbm,
    d_ref, gvall, trail,
    ru, rv, dl, du, mh, ml, cuall, cvall, guall,
    in_sem, cu_send, cu_recv, cv_send, cv_recv, gu_send, gu_recv, gv_send, gv_recv,
    row_hello, col_hello,
):
    row = lax.axis_index("row")
    col = lax.axis_index("col")
    paired = n_row % 2 == 0
    width = 2 if paired else 1
    chips = n_row // width
    core = row % width
    chip = row // width
    mate = chip * width + (1 - core) if paired else row
    nt, pieces = ru.shape[0], guall.shape[1]
    wide = nt // pieces

    near = [(step, to * width + core, back) for step, to, back in others(chip, chips)]
    near_cols = others(col, n_col)
    row_peers = ([(0, mate, 0)] if paired else []) + near

    barrier = pltpu.get_barrier_semaphore()
    for _, to, _ in row_peers:
        @pl.when(to > row)
        def _():
            pl.semaphore_signal(barrier, inc=1, device_id=(to, col), device_id_type=MESH)
    for _, to, _ in near_cols:
        @pl.when(to > col)
        def _():
            pl.semaphore_signal(barrier, inc=1, device_id=(row, to), device_id_type=MESH)

    loads = []
    for n, (src, dst) in enumerate([
        (ru_hbm, ru), (rv_hbm, rv), (cv_hbm, cvall.at[col]), (cu_hbm, cuall.at[col]),
        (dl_hbm, dl), (du_hbm, du), (trail_hbm, trail),
    ]):
        load = pltpu.make_async_copy(src, dst, in_sem.at[n])
        load.start()
        loads.append(load)

    lower_row = chip + (core if paired else 0)
    lower_col = col
    higher_row = len(row_peers) - lower_row
    higher_col = len(near_cols) - lower_col

    @pl.when(lower_row + lower_col > 0)
    def _():
        pl.semaphore_wait(barrier, lower_row + lower_col)

    for _, to, _ in row_peers:
        @pl.when(to < row)
        def _():
            pl.semaphore_signal(row_hello, inc=1, device_id=(to, col), device_id_type=MESH)
    for _, to, _ in near_cols:
        @pl.when(to < col)
        def _():
            pl.semaphore_signal(col_hello, inc=1, device_id=(row, to), device_id_type=MESH)

    def row_copy(buf, slot, send, recv, to):
        return pltpu.make_async_remote_copy(
            src_ref=buf.at[slot], dst_ref=buf.at[slot], send_sem=send, recv_sem=recv,
            device_id=(to, col), device_id_type=MESH,
        )

    def col_send(src, buf, send, recv, to):
        return pltpu.make_async_remote_copy(
            src_ref=src, dst_ref=buf.at[col], send_sem=send, recv_sem=recv,
            device_id=(row, to), device_id_type=MESH,
        )

    def cols_to(to):
        col_send(cv_hbm, cvall, cv_send, cv_recv, to).start()
        col_send(cu_hbm, cuall, cu_send, cu_recv, to).start()

    def rows_to(to, back):
        row_copy(guall, row, gu_send, gu_recv.at[back], to).start()
        row_copy(gvall, row, gv_send, gv_recv.at[back], to).start()

    for to in range(n_col):
        @pl.when(to < col)
        def _():
            cols_to(to)
    loads[0].wait()
    loads[1].wait()
    guall[row] = pack(ru[...], wide)
    gvall[row] = pack(rv[...], wide)
    for _, to, back in reversed(row_peers):
        @pl.when(to < row)
        def _():
            rows_to(to, back)

    loads[4].wait()
    loads[5].wait()
    half = order // 2
    uh, ul = split(du[...])
    lh, ll = split(dl[...])

    def product(rows, mid, cols):
        a, b = uh[rows, mid], ul[rows, mid]
        c, d = lh[mid, cols], ll[mid, cols]
        return dot(a, c) + (dot(a, d) + dot(b, c))

    lo, hi, full = slice(0, half), slice(half, order), slice(0, order)
    for rows, mid, cols in ((lo, full, lo), (lo, hi, hi), (hi, hi, lo), (hi, hi, hi)):
        mh[rows, cols], ml[rows, cols] = split(product(rows, mid, cols))

    @pl.when(higher_row > 0)
    def _():
        pl.semaphore_wait(row_hello, higher_row)
    for _, to, back in row_peers:
        @pl.when(to > row)
        def _():
            rows_to(to, back)

    @pl.when(higher_col > 0)
    def _():
        pl.semaphore_wait(col_hello, higher_col)
    for _, to, _ in near_cols:
        pl.when(to > col)(functools.partial(cols_to, to))

    def arrive(buf, slot, send, recv, step):
        row_copy(buf, slot, send, recv.at[step], mate).wait_recv()
        if paired:
            row_copy(buf, slot, send, recv.at[0], mate).start()

    for step, slot, _ in near:
        arrive(guall, slot, gu_send, gu_recv, step)
        arrive(gvall, slot, gv_send, gv_recv, step)

    def all_of(buf, count, send, recv):
        part = buf.at[pl.ds(0, count)]
        return pltpu.make_async_remote_copy(
            src_ref=part, dst_ref=part, send_sem=send, recv_sem=recv,
            device_id=(mate, col), device_id_type=MESH,
        )

    tiles = cvall.shape[1]
    loads[2].wait()
    loads[3].wait()
    loads[6].wait()
    if n_col > 1:
        all_of(cvall, n_col - 1, cv_send, cv_recv).wait_recv()
    weights = []
    for t in range(tiles):
        turned = jnp.concatenate([cvall[c, t] for c in range(n_col)], axis=-1)
        wh, wl = split(dot(turned, mh[...]) + dot(turned, ml[...]))
        weights.append(jnp.concatenate([wh, wl], axis=0))

    if n_col > 1:
        all_of(cuall, n_col - 1, cu_send, cu_recv).wait_recv()
    if paired:
        all_of(guall, chips, gu_send, gu_recv.at[0]).wait_recv()
    lanes = wide * rank
    spread = jnp.concatenate([guall[:, p].reshape(order, lanes) for p in range(pieces)], axis=-1)
    for t in range(tiles):
        turned = jnp.concatenate([cuall[c, t] for c in range(n_col)], axis=-1).astype(F32)
        left = jnp.concatenate([turned, turned], axis=0).T.astype(BF16)
        c = dot(weights[t], spread)
        ch, cl = split(c[:rank] + c[rank:])
        high, low = split(dot(left, jnp.concatenate([ch, cl], axis=0)))
        for p in range(pieces):
            at = slice(p * lanes, (p + 1) * lanes)
            d_ref[t * pieces + p] = jnp.concatenate([high[:, at], low[:, at]], axis=-1)

    if paired:
        all_of(gvall, chips, gv_send, gv_recv.at[0]).wait_recv()
    if n_col > 1:
        all_of(cvall, n_col - 1, cv_send, cv_recv).wait_send()
        all_of(cuall, n_col - 1, cu_send, cu_recv).wait_send()
    if n_row > 1:
        all_of(guall, n_row - 1, gu_send, gu_recv.at[0]).wait_send()
        all_of(gvall, n_row - 1, gv_send, gv_recv.at[0]).wait_send()


def update_kernel(blocks, rank, d_ref, gv_ref, trail, out_hbm, out, out_sem):
    n_row, pieces, rc, lanes = gv_ref.shape
    order = n_row * rc
    count = order // blocks
    wide = lanes // rank
    tiles = d_ref.shape[0] // pieces
    for p in range(pieces):
        part = gv_ref[:, p].reshape(order, lanes)
        tile_of = lax.broadcasted_iota(jnp.int32, part.shape, 1) // rank
        for w in range(wide):
            only = jnp.where(tile_of == w, part.astype(F32), 0.0).astype(BF16) if wide > 1 else part
            right = jnp.concatenate([only, only], axis=-1)
            for b in range(blocks):
                for t in range(tiles):
                    rows = pl.ds(t * order, order)
                    at = pl.ds((p * wide + w) * order + b * count, count)
                    product = dot_rt(d_ref[t * pieces + p], right[b * count:(b + 1) * count])
                    out[rows, at] = (trail[rows, at].astype(F32) - product).astype(BF16)
                    pltpu.make_async_copy(out.at[rows, at], out_hbm.at[rows, at], out_sem).start()
    pltpu.make_async_copy(out, out_hbm, out_sem).wait()


def shards(n_row, n_col, trailing, col_u, col_v, row_u, row_v, diag_lower_inv, diag_upper_inv):
    mt, cc, rank = col_u.shape
    nt, rc, _ = row_u.shape
    order = diag_lower_inv.shape[0]
    anywhere = pl.BlockSpec(memory_space=pl.ANY)
    dma = pltpu.SemaphoreType.DMA
    vmem = pl.BlockSpec(memory_space=pltpu.VMEM)
    wide = max(1, LANES // rank)
    wide = wide if nt % wide == 0 else 1
    chips = n_row // 2 if n_row % 2 == 0 else n_row
    panel = pltpu.VMEM((n_row, nt // wide, rc, wide * rank), BF16)
    handed = pl.pallas_call(
        functools.partial(panel_kernel, n_row, n_col, order, rank),
        out_shape=[
            pltpu.VMEM((mt * nt // wide, order, 2 * wide * rank), BF16),
            panel,
            pltpu.VMEM(trailing.shape, BF16),
        ],
        in_specs=[anywhere] * 7,
        out_specs=[vmem] * 3,
        scratch_shapes=[
            pltpu.VMEM(row_u.shape, BF16),
            pltpu.VMEM(row_v.shape, BF16),
            pltpu.VMEM((order, order), F32),
            pltpu.VMEM((order, order), F32),
            pltpu.VMEM((order, order), BF16),
            pltpu.VMEM((order, order), BF16),
            pltpu.VMEM((n_col, mt, rank, cc), BF16),
            pltpu.VMEM((n_col, mt, rank, cc), BF16),
            panel,
            dma((7,)), dma(()), dma(()), dma(()), dma(()),
            dma(()), dma((chips,)), dma(()), dma((chips,)),
            pltpu.SemaphoreType.REGULAR, pltpu.SemaphoreType.REGULAR,
        ],
        compiler_params=pltpu.CompilerParams(collective_id=0, has_side_effects=True),
        name="panels",
    )(
        jnp.swapaxes(col_u, 1, 2), jnp.swapaxes(col_v, 1, 2), row_u, row_v,
        diag_lower_inv, diag_upper_inv, trailing,
    )
    handed = [pltpu.with_memory_space_constraint(x, pltpu.VMEM) for x in handed]
    return pl.pallas_call(
        functools.partial(update_kernel, BLOCKS, rank),
        out_shape=jax.ShapeDtypeStruct(trailing.shape, BF16),
        in_specs=[vmem] * 3,
        out_specs=anywhere,
        scratch_shapes=[pltpu.VMEM(trailing.shape, BF16), dma(())],
        name="update",
    )(*handed)


def solution(mesh):
    placed = (
        P("row", "col"),
        P("row", "col", None),
        P("row", "col", None),
        P("col", "row", None),
        P("col", "row", None),
        P(),
        P(),
    )
    return jax.shard_map(
        functools.partial(shards, mesh.shape["row"], mesh.shape["col"]),
        mesh=mesh, in_specs=placed, out_specs=P("row", "col"), check_vma=False,
    )
```

```python
import functools

import jax
import jax.numpy as jnp
from jax import lax
from jax.experimental import pallas as pl
from jax.experimental.pallas import tpu as pltpu
from jax.sharding import PartitionSpec as P

MESH = pl.DeviceIdType.MESH
F32 = jnp.float32
BF16 = jnp.bfloat16
LANES = 128
BLOCKS = 1


def others(at, count):
    if count & (count - 1):
        return [(step, lax.rem(at + step, count), count - step) for step in range(1, count)]
    out = []
    for step in range(1, count):
        to, weight = jnp.int32(0), 1
        while weight < count:
            bit = (at // weight) % 2
            to = to + weight * ((1 - bit) if step & weight else bit)
            weight *= 2
        out.append((step, to, step))
    return out


def split(x):
    high = x.astype(BF16)
    return high, (x - high.astype(F32)).astype(BF16)


def dot(a, b):
    return lax.dot_general(a, b, (((1,), (0,)), ((), ())), preferred_element_type=F32)


def dot_rt(a, b):
    return lax.dot_general(a, b, (((1,), (1,)), ((), ())), preferred_element_type=F32)


def pack(x, width):
    if width == 1:
        return x
    x = x.astype(F32)
    return jnp.stack([
        jnp.concatenate([x[p * width + w] for w in range(width)], axis=-1)
        for p in range(x.shape[0] // width)
    ]).astype(BF16)


def panel_kernel(
    n_row, n_col, order, rank,
    cu_hbm, cv_hbm, ru_hbm, rv_hbm, dl_hbm, du_hbm, trail_hbm,
    d_ref, gvall, trail,
    own, diag, mh, ml, cuall, cvall, guall,
    in_sem, cu_send, cu_recv, cv_send, cv_recv, gu_send, gu_recv, gv_send, gv_recv,
    row_hello, col_hello,
):
    row = lax.axis_index("row")
    col = lax.axis_index("col")
    paired = n_row % 2 == 0
    width = 2 if paired else 1
    chips = n_row // width
    core = row % width
    chip = row // width
    mate = chip * width + (1 - core) if paired else row
    nt, pieces = own.shape[1], guall.shape[1]
    wide = nt // pieces

    near = [(step, to * width + core, back) for step, to, back in others(chip, chips)]
    near_cols = others(col, n_col)
    row_peers = ([(0, mate, 0)] if paired else []) + near

    def load(src, dst, sem):
        copy = pltpu.make_async_copy(src, dst, sem)
        copy.start()
        return copy

    load(ru_hbm, own.at[0], in_sem.at[0])
    load(rv_hbm, own.at[1], in_sem.at[0])
    load(cv_hbm, cvall.at[col], cv_recv)
    load(cu_hbm, cuall.at[col], cu_recv)

    barrier = pltpu.get_barrier_semaphore()
    for _, to, _ in row_peers:
        @pl.when(to > row)
        def _():
            pl.semaphore_signal(barrier, inc=1, device_id=(to, col), device_id_type=MESH)
    for _, to, _ in near_cols:
        @pl.when(to > col)
        def _():
            pl.semaphore_signal(barrier, inc=1, device_id=(row, to), device_id_type=MESH)

    load(dl_hbm, diag.at[0], in_sem.at[1])
    load(du_hbm, diag.at[1], in_sem.at[1])
    trail_load = load(trail_hbm, trail, in_sem.at[2])

    lower_row = chip + (core if paired else 0)
    lower_col = col
    higher_row = len(row_peers) - lower_row
    higher_col = len(near_cols) - lower_col

    @pl.when(lower_row + lower_col > 0)
    def _():
        pl.semaphore_wait(barrier, lower_row + lower_col)

    def row_copy(buf, slot, send, recv, to):
        return pltpu.make_async_remote_copy(
            src_ref=buf.at[slot], dst_ref=buf.at[slot], send_sem=send, recv_sem=recv,
            device_id=(to, col), device_id_type=MESH,
        )

    def col_send(src, buf, send, recv, to):
        return pltpu.make_async_remote_copy(
            src_ref=src, dst_ref=buf.at[col], send_sem=send, recv_sem=recv,
            device_id=(row, to), device_id_type=MESH,
        )

    def cols_to(to):
        col_send(cv_hbm, cvall, cv_send, cv_recv, to).start()
        col_send(cu_hbm, cuall, cu_send, cu_recv, to).start()

    def rows_to(to, back):
        row_copy(guall, row, gu_send, gu_recv.at[back], to).start()
        row_copy(gvall, row, gv_send, gv_recv.at[back], to).start()

    for to in range(n_col):
        @pl.when(to < col)
        def _():
            cols_to(to)
    for _, to, _ in row_peers:
        @pl.when(to < row)
        def _():
            pl.semaphore_signal(row_hello, inc=1, device_id=(to, col), device_id_type=MESH)
    for _, to, _ in near_cols:
        @pl.when(to < col)
        def _():
            pl.semaphore_signal(col_hello, inc=1, device_id=(row, to), device_id_type=MESH)

    pltpu.make_async_copy(own, own, in_sem.at[0]).wait()
    guall[row] = pack(own[0], wide)
    gvall[row] = pack(own[1], wide)
    for _, to, back in reversed(row_peers):
        @pl.when(to < row)
        def _():
            rows_to(to, back)

    @pl.when(higher_row > 0)
    def _():
        pl.semaphore_wait(row_hello, higher_row)
    for _, to, back in row_peers:
        @pl.when(to > row)
        def _():
            rows_to(to, back)

    @pl.when(higher_col > 0)
    def _():
        pl.semaphore_wait(col_hello, higher_col)
    for _, to, _ in near_cols:
        pl.when(to > col)(functools.partial(cols_to, to))

    pltpu.make_async_copy(diag, diag, in_sem.at[1]).wait()
    half = order // 2
    uh, ul = split(diag[1])
    lh, ll = split(diag[0])

    def product(rows, mid, cols):
        a, b = uh[rows, mid], ul[rows, mid]
        c, d = lh[mid, cols], ll[mid, cols]
        return dot(a, c) + (dot(a, d) + dot(b, c))

    lo, hi, full = slice(0, half), slice(half, order), slice(0, order)
    for rows, mid, cols in ((lo, full, lo), (lo, hi, hi), (hi, hi, lo), (hi, hi, hi)):
        mh[rows, cols], ml[rows, cols] = split(product(rows, mid, cols))

    def arrive(buf, slot, send, recv, step):
        row_copy(buf, slot, send, recv.at[step], mate).wait_recv()
        if paired:
            row_copy(buf, slot, send, recv.at[0], mate).start()

    for step, slot, _ in near:
        arrive(guall, slot, gu_send, gu_recv, step)
    for step, slot, _ in near:
        arrive(gvall, slot, gv_send, gv_recv, step)

    def all_of(buf, count, send, recv):
        part = buf.at[pl.ds(0, count)]
        return pltpu.make_async_remote_copy(
            src_ref=part, dst_ref=part, send_sem=send, recv_sem=recv,
            device_id=(mate, col), device_id_type=MESH,
        )

    tiles = cvall.shape[1]
    trail_load.wait()
    all_of(cvall, n_col, cv_send, cv_recv).wait_recv()
    weights = []
    for t in range(tiles):
        turned = jnp.concatenate([cvall[c, t] for c in range(n_col)], axis=-1)
        wh, wl = split(dot(turned, mh[...]) + dot(turned, ml[...]))
        weights.append(jnp.concatenate([wh, wl], axis=0))

    all_of(cuall, n_col, cu_send, cu_recv).wait_recv()
    if paired:
        all_of(guall, chips, gu_send, gu_recv.at[0]).wait_recv()
    lanes = wide * rank
    spread = jnp.concatenate([guall[:, p].reshape(order, lanes) for p in range(pieces)], axis=-1)
    for t in range(tiles):
        turned = jnp.concatenate([cuall[c, t] for c in range(n_col)], axis=-1).astype(F32)
        left = jnp.concatenate([turned, turned], axis=0).T.astype(BF16)
        c = dot(weights[t], spread)
        ch, cl = split(c[:rank] + c[rank:])
        high, low = split(dot(left, jnp.concatenate([ch, cl], axis=0)))
        for p in range(pieces):
            at = slice(p * lanes, (p + 1) * lanes)
            d_ref[t * pieces + p] = jnp.concatenate([high[:, at], low[:, at]], axis=-1)

    if paired:
        all_of(gvall, chips, gv_send, gv_recv.at[0]).wait_recv()
    if n_col > 1:
        all_of(cvall, n_col - 1, cv_send, cv_recv).wait_send()
        all_of(cuall, n_col - 1, cu_send, cu_recv).wait_send()
    if n_row > 1:
        all_of(guall, n_row - 1, gu_send, gu_recv.at[0]).wait_send()
        all_of(gvall, n_row - 1, gv_send, gv_recv.at[0]).wait_send()


def update_kernel(blocks, rank, d_ref, gv_ref, trail, out_hbm, out, out_sem):
    n_row, pieces, rc, lanes = gv_ref.shape
    order = n_row * rc
    count = order // blocks
    wide = lanes // rank
    tiles = d_ref.shape[0] // pieces
    for p in range(pieces):
        part = gv_ref[:, p].reshape(order, lanes)
        tile_of = lax.broadcasted_iota(jnp.int32, part.shape, 1) // rank
        for w in range(wide):
            only = jnp.where(tile_of == w, part.astype(F32), 0.0).astype(BF16) if wide > 1 else part
            right = jnp.concatenate([only, only], axis=-1)
            for b in range(blocks):
                for t in range(tiles):
                    rows = pl.ds(t * order, order)
                    at = pl.ds((p * wide + w) * order + b * count, count)
                    product = dot_rt(d_ref[t * pieces + p], right[b * count:(b + 1) * count])
                    out[rows, at] = (trail[rows, at].astype(F32) - product).astype(BF16)
                    pltpu.make_async_copy(out.at[rows, at], out_hbm.at[rows, at], out_sem).start()
    pltpu.make_async_copy(out, out_hbm, out_sem).wait()


def shards(n_row, n_col, trailing, col_u, col_v, row_u, row_v, diag_lower_inv, diag_upper_inv):
    mt, cc, rank = col_u.shape
    nt, rc, _ = row_u.shape
    order = diag_lower_inv.shape[0]
    anywhere = pl.BlockSpec(memory_space=pl.ANY)
    dma = pltpu.SemaphoreType.DMA
    vmem = pl.BlockSpec(memory_space=pltpu.VMEM)
    wide = max(1, LANES // rank)
    wide = wide if nt % wide == 0 else 1
    chips = n_row // 2 if n_row % 2 == 0 else n_row
    panel = pltpu.VMEM((n_row, nt // wide, rc, wide * rank), BF16)
    handed = pl.pallas_call(
        functools.partial(panel_kernel, n_row, n_col, order, rank),
        out_shape=[
            pltpu.VMEM((mt * nt // wide, order, 2 * wide * rank), BF16),
            panel,
            pltpu.VMEM(trailing.shape, BF16),
        ],
        in_specs=[anywhere] * 7,
        out_specs=[vmem] * 3,
        scratch_shapes=[
            pltpu.VMEM((2, *row_u.shape), BF16),
            pltpu.VMEM((2, order, order), F32),
            pltpu.VMEM((order, order), BF16),
            pltpu.VMEM((order, order), BF16),
            pltpu.VMEM((n_col, mt, rank, cc), BF16),
            pltpu.VMEM((n_col, mt, rank, cc), BF16),
            panel,
            dma((3,)), dma(()), dma(()), dma(()), dma(()),
            dma(()), dma((chips,)), dma(()), dma((chips,)),
            pltpu.SemaphoreType.REGULAR, pltpu.SemaphoreType.REGULAR,
        ],
        compiler_params=pltpu.CompilerParams(collective_id=0, has_side_effects=True),
        name="panels",
    )(
        jnp.swapaxes(col_u, 1, 2), jnp.swapaxes(col_v, 1, 2), row_u, row_v,
        diag_lower_inv, diag_upper_inv, trailing,
    )
    handed = [pltpu.with_memory_space_constraint(x, pltpu.VMEM) for x in handed]
    return pl.pallas_call(
        functools.partial(update_kernel, BLOCKS, rank),
        out_shape=jax.ShapeDtypeStruct(trailing.shape, BF16),
        in_specs=[vmem] * 3,
        out_specs=anywhere,
        scratch_shapes=[pltpu.VMEM(trailing.shape, BF16), dma(())],
        name="update",
    )(*handed)


def solution(mesh):
    placed = (
        P("row", "col"),
        P("row", "col", None),
        P("row", "col", None),
        P("col", "row", None),
        P("col", "row", None),
        P(),
        P(),
    )
    return jax.shard_map(
        functools.partial(shards, mesh.shape["row"], mesh.shape["col"]),
        mesh=mesh, in_specs=placed, out_specs=P("row", "col"), check_vma=False,
    )
```

```python
import functools

import jax
import jax.numpy as jnp
from jax import lax
from jax.experimental import pallas as pl
from jax.experimental.pallas import tpu as pltpu
from jax.sharding import PartitionSpec as P

MESH = pl.DeviceIdType.MESH
F32 = jnp.float32
BF16 = jnp.bfloat16
LANES = 128
BLOCKS = 1


def others(at, count):
    if count & (count - 1):
        return [(step, lax.rem(at + step, count), count - step) for step in range(1, count)]
    out = []
    for step in range(1, count):
        to, weight = jnp.int32(0), 1
        while weight < count:
            bit = (at // weight) % 2
            to = to + weight * ((1 - bit) if step & weight else bit)
            weight *= 2
        out.append((step, to, step))
    return out


def split(x):
    high = x.astype(BF16)
    return high, (x - high.astype(F32)).astype(BF16)


def dot(a, b):
    return lax.dot_general(a, b, (((1,), (0,)), ((), ())), preferred_element_type=F32)


def dot_rt(a, b):
    return lax.dot_general(a, b, (((1,), (1,)), ((), ())), preferred_element_type=F32)


def pack(x, width):
    if width == 1:
        return x
    x = x.astype(F32)
    return jnp.stack([
        jnp.concatenate([x[p * width + w] for w in range(width)], axis=-1)
        for p in range(x.shape[0] // width)
    ]).astype(BF16)


def panel_kernel(
    n_row, n_col, order, rank,
    cu_hbm, cv_hbm, ru_hbm, rv_hbm, dl_hbm, du_hbm, trail_hbm,
    d_ref, gvall, trail,
    own, diag, mh, ml, cuall, cvall, guall,
    in_sem, cu_send, cu_recv, cv_send, cv_recv, gu_send, gu_recv, gv_send, gv_recv,
    row_hello, col_hello,
):
    row = lax.axis_index("row")
    col = lax.axis_index("col")
    paired = n_row % 2 == 0
    width = 2 if paired else 1
    chips = n_row // width
    core = row % width
    chip = row // width
    mate = chip * width + (1 - core) if paired else row
    nt, pieces = own.shape[1], guall.shape[1]
    wide = nt // pieces

    near = [(step, to * width + core, back) for step, to, back in others(chip, chips)]
    near_cols = others(col, n_col)
    row_peers = ([(0, mate, 0)] if paired else []) + near

    def load(src, dst, sem):
        copy = pltpu.make_async_copy(src, dst, sem)
        copy.start()
        return copy

    load(ru_hbm, own.at[0], in_sem.at[0])
    load(rv_hbm, own.at[1], in_sem.at[0])
    cv_load = load(cv_hbm, cvall.at[col], in_sem.at[3])
    cu_load = load(cu_hbm, cuall.at[col], in_sem.at[4])

    barrier = pltpu.get_barrier_semaphore()
    for _, to, _ in row_peers:
        @pl.when(to > row)
        def _():
            pl.semaphore_signal(barrier, inc=1, device_id=(to, col), device_id_type=MESH)
    for _, to, _ in near_cols:
        @pl.when(to > col)
        def _():
            pl.semaphore_signal(barrier, inc=1, device_id=(row, to), device_id_type=MESH)

    load(dl_hbm, diag.at[0], in_sem.at[1])
    load(du_hbm, diag.at[1], in_sem.at[1])
    trail_load = load(trail_hbm, trail, in_sem.at[2])

    lower_row = chip + (core if paired else 0)
    lower_col = col
    higher_row = len(row_peers) - lower_row
    higher_col = len(near_cols) - lower_col

    @pl.when(lower_row + lower_col > 0)
    def _():
        pl.semaphore_wait(barrier, lower_row + lower_col)

    def row_copy(buf, slot, send, recv, to):
        return pltpu.make_async_remote_copy(
            src_ref=buf.at[slot], dst_ref=buf.at[slot], send_sem=send, recv_sem=recv,
            device_id=(to, col), device_id_type=MESH,
        )

    def col_send(src, buf, send, recv, to):
        return pltpu.make_async_remote_copy(
            src_ref=src, dst_ref=buf.at[col], send_sem=send, recv_sem=recv,
            device_id=(row, to), device_id_type=MESH,
        )

    def cols_to(to, cv, cu):
        col_send(cv, cvall, cv_send, cv_recv, to).start()
        col_send(cu, cuall, cu_send, cu_recv, to).start()

    def rows_to(to, back):
        row_copy(guall, row, gu_send, gu_recv.at[back], to).start()
        row_copy(gvall, row, gv_send, gv_recv.at[back], to).start()

    for to in range(n_col):
        @pl.when(to < col)
        def _():
            cols_to(to, cv_hbm, cu_hbm)
    for _, to, _ in row_peers:
        @pl.when(to < row)
        def _():
            pl.semaphore_signal(row_hello, inc=1, device_id=(to, col), device_id_type=MESH)
    for _, to, _ in near_cols:
        @pl.when(to < col)
        def _():
            pl.semaphore_signal(col_hello, inc=1, device_id=(row, to), device_id_type=MESH)

    pltpu.make_async_copy(own, own, in_sem.at[0]).wait()
    guall[row] = pack(own[0], wide)
    gvall[row] = pack(own[1], wide)
    for _, to, back in reversed(row_peers):
        @pl.when(to < row)
        def _():
            rows_to(to, back)

    @pl.when(higher_row > 0)
    def _():
        pl.semaphore_wait(row_hello, higher_row)
    for _, to, back in row_peers:
        @pl.when(to > row)
        def _():
            rows_to(to, back)

    cv_load.wait()
    cu_load.wait()

    @pl.when(higher_col > 0)
    def _():
        pl.semaphore_wait(col_hello, higher_col)
    for _, to, _ in near_cols:
        pl.when(to > col)(functools.partial(cols_to, to, cvall.at[col], cuall.at[col]))

    pltpu.make_async_copy(diag, diag, in_sem.at[1]).wait()
    half = order // 2
    uh, ul = split(diag[1])
    lh, ll = split(diag[0])

    def product(rows, mid, cols):
        a, b = uh[rows, mid], ul[rows, mid]
        c, d = lh[mid, cols], ll[mid, cols]
        return dot(a, c) + (dot(a, d) + dot(b, c))

    lo, hi, full = slice(0, half), slice(half, order), slice(0, order)
    for rows, mid, cols in ((lo, full, lo), (lo, hi, hi), (hi, hi, lo), (hi, hi, hi)):
        mh[rows, cols], ml[rows, cols] = split(product(rows, mid, cols))

    def arrive(buf, slot, send, recv, step):
        row_copy(buf, slot, send, recv.at[step], mate).wait_recv()
        if paired:
            row_copy(buf, slot, send, recv.at[0], mate).start()

    for step, slot, _ in near:
        arrive(guall, slot, gu_send, gu_recv, step)
    for step, slot, _ in near:
        arrive(gvall, slot, gv_send, gv_recv, step)

    def all_of(buf, count, send, recv):
        part = buf.at[pl.ds(0, count)]
        return pltpu.make_async_remote_copy(
            src_ref=part, dst_ref=part, send_sem=send, recv_sem=recv,
            device_id=(mate, col), device_id_type=MESH,
        )

    tiles = cvall.shape[1]
    trail_load.wait()
    if n_col > 1:
        all_of(cvall, n_col - 1, cv_send, cv_recv).wait_recv()
    weights = []
    for t in range(tiles):
        turned = jnp.concatenate([cvall[c, t] for c in range(n_col)], axis=-1)
        wh, wl = split(dot(turned, mh[...]) + dot(turned, ml[...]))
        weights.append(jnp.concatenate([wh, wl], axis=0))

    if n_col > 1:
        all_of(cuall, n_col - 1, cu_send, cu_recv).wait_recv()
    if paired:
        all_of(guall, chips, gu_send, gu_recv.at[0]).wait_recv()
    lanes = wide * rank
    spread = jnp.concatenate([guall[:, p].reshape(order, lanes) for p in range(pieces)], axis=-1)
    for t in range(tiles):
        turned = jnp.concatenate([cuall[c, t] for c in range(n_col)], axis=-1).astype(F32)
        left = jnp.concatenate([turned, turned], axis=0).T.astype(BF16)
        c = dot(weights[t], spread)
        ch, cl = split(c[:rank] + c[rank:])
        high, low = split(dot(left, jnp.concatenate([ch, cl], axis=0)))
        for p in range(pieces):
            at = slice(p * lanes, (p + 1) * lanes)
            d_ref[t * pieces + p] = jnp.concatenate([high[:, at], low[:, at]], axis=-1)

    if paired:
        all_of(gvall, chips, gv_send, gv_recv.at[0]).wait_recv()
    if n_col > 1:
        all_of(cvall, n_col - 1, cv_send, cv_recv).wait_send()
        all_of(cuall, n_col - 1, cu_send, cu_recv).wait_send()
    if n_row > 1:
        all_of(guall, n_row - 1, gu_send, gu_recv.at[0]).wait_send()
        all_of(gvall, n_row - 1, gv_send, gv_recv.at[0]).wait_send()


def update_kernel(blocks, rank, d_ref, gv_ref, trail, out_hbm, out, out_sem):
    n_row, pieces, rc, lanes = gv_ref.shape
    order = n_row * rc
    count = order // blocks
    wide = lanes // rank
    tiles = d_ref.shape[0] // pieces
    for p in range(pieces):
        part = gv_ref[:, p].reshape(order, lanes)
        tile_of = lax.broadcasted_iota(jnp.int32, part.shape, 1) // rank
        for w in range(wide):
            only = jnp.where(tile_of == w, part.astype(F32), 0.0).astype(BF16) if wide > 1 else part
            right = jnp.concatenate([only, only], axis=-1)
            for b in range(blocks):
                for t in range(tiles):
                    rows = pl.ds(t * order, order)
                    at = pl.ds((p * wide + w) * order + b * count, count)
                    product = dot_rt(d_ref[t * pieces + p], right[b * count:(b + 1) * count])
                    out[rows, at] = (trail[rows, at].astype(F32) - product).astype(BF16)
                    pltpu.make_async_copy(out.at[rows, at], out_hbm.at[rows, at], out_sem).start()
    pltpu.make_async_copy(out, out_hbm, out_sem).wait()


def shards(n_row, n_col, trailing, col_u, col_v, row_u, row_v, diag_lower_inv, diag_upper_inv):
    mt, cc, rank = col_u.shape
    nt, rc, _ = row_u.shape
    order = diag_lower_inv.shape[0]
    anywhere = pl.BlockSpec(memory_space=pl.ANY)
    dma = pltpu.SemaphoreType.DMA
    vmem = pl.BlockSpec(memory_space=pltpu.VMEM)
    wide = max(1, LANES // rank)
    wide = wide if nt % wide == 0 else 1
    chips = n_row // 2 if n_row % 2 == 0 else n_row
    panel = pltpu.VMEM((n_row, nt // wide, rc, wide * rank), BF16)
    handed = pl.pallas_call(
        functools.partial(panel_kernel, n_row, n_col, order, rank),
        out_shape=[
            pltpu.VMEM((mt * nt // wide, order, 2 * wide * rank), BF16),
            panel,
            pltpu.VMEM(trailing.shape, BF16),
        ],
        in_specs=[anywhere] * 7,
        out_specs=[vmem] * 3,
        scratch_shapes=[
            pltpu.VMEM((2, *row_u.shape), BF16),
            pltpu.VMEM((2, order, order), F32),
            pltpu.VMEM((order, order), BF16),
            pltpu.VMEM((order, order), BF16),
            pltpu.VMEM((n_col, mt, rank, cc), BF16),
            pltpu.VMEM((n_col, mt, rank, cc), BF16),
            panel,
            dma((5,)), dma(()), dma(()), dma(()), dma(()),
            dma(()), dma((chips,)), dma(()), dma((chips,)),
            pltpu.SemaphoreType.REGULAR, pltpu.SemaphoreType.REGULAR,
        ],
        compiler_params=pltpu.CompilerParams(collective_id=0, has_side_effects=True),
        name="panels",
    )(
        jnp.swapaxes(col_u, 1, 2), jnp.swapaxes(col_v, 1, 2), row_u, row_v,
        diag_lower_inv, diag_upper_inv, trailing,
    )
    handed = [pltpu.with_memory_space_constraint(x, pltpu.VMEM) for x in handed]
    return pl.pallas_call(
        functools.partial(update_kernel, BLOCKS, rank),
        out_shape=jax.ShapeDtypeStruct(trailing.shape, BF16),
        in_specs=[vmem] * 3,
        out_specs=anywhere,
        scratch_shapes=[pltpu.VMEM(trailing.shape, BF16), dma(())],
        name="update",
    )(*handed)


def solution(mesh):
    placed = (
        P("row", "col"),
        P("row", "col", None),
        P("row", "col", None),
        P("col", "row", None),
        P("col", "row", None),
        P(),
        P(),
    )
    return jax.shard_map(
        functools.partial(shards, mesh.shape["row"], mesh.shape["col"]),
        mesh=mesh, in_specs=placed, out_specs=P("row", "col"), check_vma=False,
    )
```

```python
import functools

import jax
import jax.numpy as jnp
from jax import lax
from jax.experimental import pallas as pl
from jax.experimental.pallas import tpu as pltpu
from jax.sharding import PartitionSpec as P

MESH = pl.DeviceIdType.MESH
F32 = jnp.float32
BF16 = jnp.bfloat16
LANES = 128
BLOCKS = 1


def others(at, count):
    if count & (count - 1):
        return [(step, lax.rem(at + step, count), count - step) for step in range(1, count)]
    out = []
    for step in range(1, count):
        to, weight = jnp.int32(0), 1
        while weight < count:
            bit = (at // weight) % 2
            to = to + weight * ((1 - bit) if step & weight else bit)
            weight *= 2
        out.append((step, to, step))
    return out


def split(x):
    high = x.astype(BF16)
    return high, (x - high.astype(F32)).astype(BF16)


def dot(a, b):
    return lax.dot_general(a, b, (((1,), (0,)), ((), ())), preferred_element_type=F32)


def dot_rt(a, b):
    return lax.dot_general(a, b, (((1,), (1,)), ((), ())), preferred_element_type=F32)


def pack(x, width):
    if width == 1:
        return x
    x = x.astype(F32)
    return jnp.stack([
        jnp.concatenate([x[p * width + w] for w in range(width)], axis=-1)
        for p in range(x.shape[0] // width)
    ]).astype(BF16)


def panel_kernel(
    n_row, n_col, order, rank,
    cu_hbm, cv_hbm, ru_hbm, rv_hbm, dl_hbm, du_hbm, trail_hbm,
    d_ref, gvall, trail,
    own, diag, mh, ml, cuall, cvall, guall,
    in_sem, cu_send, cu_recv, cv_send, cv_recv, gu_send, gu_recv, gv_send, gv_recv,
    row_hello, col_hello,
):
    row = lax.axis_index("row")
    col = lax.axis_index("col")
    paired = n_row % 2 == 0
    width = 2 if paired else 1
    chips = n_row // width
    core = row % width
    chip = row // width
    mate = chip * width + (1 - core) if paired else row
    nt, pieces = own.shape[1], guall.shape[1]
    wide = nt // pieces

    near = [(step, to * width + core, back) for step, to, back in others(chip, chips)]
    near_cols = others(col, n_col)
    row_peers = ([(0, mate, 0)] if paired else []) + near

    def load(src, dst, sem):
        copy = pltpu.make_async_copy(src, dst, sem)
        copy.start()
        return copy

    load(ru_hbm, own.at[0], in_sem.at[0])
    load(rv_hbm, own.at[1], in_sem.at[0])
    cv_load = load(cv_hbm, cvall.at[col], in_sem.at[3])
    cu_load = load(cu_hbm, cuall.at[col], in_sem.at[4])

    barrier = pltpu.get_barrier_semaphore()
    for _, to, _ in row_peers:
        @pl.when(to > row)
        def _():
            pl.semaphore_signal(barrier, inc=1, device_id=(to, col), device_id_type=MESH)
    for _, to, _ in near_cols:
        @pl.when(to > col)
        def _():
            pl.semaphore_signal(barrier, inc=1, device_id=(row, to), device_id_type=MESH)

    load(dl_hbm, diag.at[0], in_sem.at[1])
    load(du_hbm, diag.at[1], in_sem.at[1])
    trail_load = load(trail_hbm, trail, in_sem.at[2])

    lower_row = chip + (core if paired else 0)
    lower_col = col

    @pl.when(lower_row + lower_col > 0)
    def _():
        pl.semaphore_wait(barrier, lower_row + lower_col)

    def row_copy(buf, slot, send, recv, to):
        return pltpu.make_async_remote_copy(
            src_ref=buf.at[slot], dst_ref=buf.at[slot], send_sem=send, recv_sem=recv,
            device_id=(to, col), device_id_type=MESH,
        )

    def col_send(src, buf, send, recv, to):
        return pltpu.make_async_remote_copy(
            src_ref=src, dst_ref=buf.at[col], send_sem=send, recv_sem=recv,
            device_id=(row, to), device_id_type=MESH,
        )

    def cols_to(to, cv, cu):
        col_send(cv, cvall, cv_send, cv_recv, to).start()
        col_send(cu, cuall, cu_send, cu_recv, to).start()

    def rows_to(to, back):
        row_copy(guall, row, gu_send, gu_recv.at[back], to).start()
        row_copy(gvall, row, gv_send, gv_recv.at[back], to).start()

    for to in range(n_col):
        @pl.when(to < col)
        def _():
            cols_to(to, cv_hbm, cu_hbm)
    for _, to, back in row_peers:
        @pl.when(to < row)
        def _():
            pl.semaphore_signal(row_hello.at[back], inc=1, device_id=(to, col), device_id_type=MESH)
    for _, to, back in near_cols:
        @pl.when(to < col)
        def _():
            pl.semaphore_signal(col_hello.at[back], inc=1, device_id=(row, to), device_id_type=MESH)

    pltpu.make_async_copy(own, own, in_sem.at[0]).wait()
    guall[row] = pack(own[0], wide)
    gvall[row] = pack(own[1], wide)
    for _, to, back in reversed(row_peers):
        @pl.when(to < row)
        def _():
            rows_to(to, back)

    cv_load.wait()
    cu_load.wait()

    def greeted_row(step, to, back):
        @pl.when(to > row)
        def _():
            pl.semaphore_wait(row_hello.at[step], 1)
            rows_to(to, back)

    def greeted_col(step, to):
        @pl.when(to > col)
        def _():
            pl.semaphore_wait(col_hello.at[step], 1)
            cols_to(to, cvall.at[col], cuall.at[col])

    if paired:
        greeted_row(0, mate, 0)
    for n in range(max(len(near), len(near_cols))):
        if n == 0 and len(near) > 1:
            greeted_row(*near[0])
            greeted_row(*near[1])
        elif n > 0 and n + 1 < len(near):
            greeted_row(*near[n + 1])
        elif n == 0 and near:
            greeted_row(*near[0])
        if n < len(near_cols):
            greeted_col(*near_cols[n][:2])

    pltpu.make_async_copy(diag, diag, in_sem.at[1]).wait()
    half = order // 2
    uh, ul = split(diag[1])
    lh, ll = split(diag[0])

    def product(rows, mid, cols):
        a, b = uh[rows, mid], ul[rows, mid]
        c, d = lh[mid, cols], ll[mid, cols]
        return dot(a, c) + (dot(a, d) + dot(b, c))

    lo, hi, full = slice(0, half), slice(half, order), slice(0, order)
    for rows, mid, cols in ((lo, full, lo), (lo, hi, hi), (hi, hi, lo), (hi, hi, hi)):
        mh[rows, cols], ml[rows, cols] = split(product(rows, mid, cols))

    def arrive(buf, slot, send, recv, step):
        row_copy(buf, slot, send, recv.at[step], mate).wait_recv()
        if paired:
            row_copy(buf, slot, send, recv.at[0], mate).start()

    for step, slot, _ in near:
        arrive(guall, slot, gu_send, gu_recv, step)
    for step, slot, _ in near:
        arrive(gvall, slot, gv_send, gv_recv, step)

    def all_of(buf, count, send, recv):
        part = buf.at[pl.ds(0, count)]
        return pltpu.make_async_remote_copy(
            src_ref=part, dst_ref=part, send_sem=send, recv_sem=recv,
            device_id=(mate, col), device_id_type=MESH,
        )

    tiles = cvall.shape[1]
    trail_load.wait()
    if n_col > 1:
        all_of(cvall, n_col - 1, cv_send, cv_recv).wait_recv()
    weights = []
    for t in range(tiles):
        turned = jnp.concatenate([cvall[c, t] for c in range(n_col)], axis=-1)
        wh, wl = split(dot(turned, mh[...]) + dot(turned, ml[...]))
        weights.append(jnp.concatenate([wh, wl], axis=0))

    if n_col > 1:
        all_of(cuall, n_col - 1, cu_send, cu_recv).wait_recv()
    if paired:
        all_of(guall, chips, gu_send, gu_recv.at[0]).wait_recv()
    lanes = wide * rank
    spread = jnp.concatenate([guall[:, p].reshape(order, lanes) for p in range(pieces)], axis=-1)
    for t in range(tiles):
        turned = jnp.concatenate([cuall[c, t] for c in range(n_col)], axis=-1).astype(F32)
        left = jnp.concatenate([turned, turned], axis=0).T.astype(BF16)
        c = dot(weights[t], spread)
        ch, cl = split(c[:rank] + c[rank:])
        high = dot(left, jnp.concatenate([ch, cl], axis=0)).astype(BF16)
        for p in range(pieces):
            at = slice(p * lanes, (p + 1) * lanes)
            d_ref[t * pieces + p] = high[:, at]

    if paired:
        all_of(gvall, chips, gv_send, gv_recv.at[0]).wait_recv()
    if n_col > 1:
        all_of(cvall, n_col - 1, cv_send, cv_recv).wait_send()
        all_of(cuall, n_col - 1, cu_send, cu_recv).wait_send()
    if n_row > 1:
        all_of(guall, n_row - 1, gu_send, gu_recv.at[0]).wait_send()
        all_of(gvall, n_row - 1, gv_send, gv_recv.at[0]).wait_send()


def update_kernel(blocks, rank, d_ref, gv_ref, trail, out_hbm, out, out_sem):
    n_row, pieces, rc, lanes = gv_ref.shape
    order = n_row * rc
    count = order // blocks
    wide = lanes // rank
    tiles = d_ref.shape[0] // pieces
    for p in range(pieces):
        part = gv_ref[:, p].reshape(order, lanes)
        tile_of = lax.broadcasted_iota(jnp.int32, part.shape, 1) // rank
        for w in range(wide):
            only = jnp.where(tile_of == w, part.astype(F32), 0.0).astype(BF16) if wide > 1 else part
            right = only
            for b in range(blocks):
                for t in range(tiles):
                    rows = pl.ds(t * order, order)
                    at = pl.ds((p * wide + w) * order + b * count, count)
                    product = dot_rt(d_ref[t * pieces + p], right[b * count:(b + 1) * count])
                    out[rows, at] = (trail[rows, at].astype(F32) - product).astype(BF16)
                    pltpu.make_async_copy(out.at[rows, at], out_hbm.at[rows, at], out_sem).start()
    pltpu.make_async_copy(out, out_hbm, out_sem).wait()


def shards(n_row, n_col, trailing, col_u, col_v, row_u, row_v, diag_lower_inv, diag_upper_inv):
    mt, cc, rank = col_u.shape
    nt, rc, _ = row_u.shape
    order = diag_lower_inv.shape[0]
    anywhere = pl.BlockSpec(memory_space=pl.ANY)
    dma = pltpu.SemaphoreType.DMA
    vmem = pl.BlockSpec(memory_space=pltpu.VMEM)
    wide = max(1, LANES // rank)
    wide = wide if nt % wide == 0 else 1
    chips = n_row // 2 if n_row % 2 == 0 else n_row
    panel = pltpu.VMEM((n_row, nt // wide, rc, wide * rank), BF16)
    handed = pl.pallas_call(
        functools.partial(panel_kernel, n_row, n_col, order, rank),
        out_shape=[
            pltpu.VMEM((mt * nt // wide, order, wide * rank), BF16),
            panel,
            pltpu.VMEM(trailing.shape, BF16),
        ],
        in_specs=[anywhere] * 7,
        out_specs=[vmem] * 3,
        scratch_shapes=[
            pltpu.VMEM((2, *row_u.shape), BF16),
            pltpu.VMEM((2, order, order), F32),
            pltpu.VMEM((order, order), BF16),
            pltpu.VMEM((order, order), BF16),
            pltpu.VMEM((n_col, mt, rank, cc), BF16),
            pltpu.VMEM((n_col, mt, rank, cc), BF16),
            panel,
            dma((5,)), dma(()), dma(()), dma(()), dma(()),
            dma(()), dma((chips,)), dma(()), dma((chips,)),
            pltpu.SemaphoreType.REGULAR((chips,)), pltpu.SemaphoreType.REGULAR((n_col,)),
        ],
        compiler_params=pltpu.CompilerParams(collective_id=0, has_side_effects=True),
        name="panels",
    )(
        jnp.swapaxes(col_u, 1, 2), jnp.swapaxes(col_v, 1, 2), row_u, row_v,
        diag_lower_inv, diag_upper_inv, trailing,
    )
    handed = [pltpu.with_memory_space_constraint(x, pltpu.VMEM) for x in handed]
    return pl.pallas_call(
        functools.partial(update_kernel, BLOCKS, rank),
        out_shape=jax.ShapeDtypeStruct(trailing.shape, BF16),
        in_specs=[vmem] * 3,
        out_specs=anywhere,
        scratch_shapes=[pltpu.VMEM(trailing.shape, BF16), dma(())],
        name="update",
    )(*handed)


def solution(mesh):
    placed = (
        P("row", "col"),
        P("row", "col", None),
        P("row", "col", None),
        P("col", "row", None),
        P("col", "row", None),
        P(),
        P(),
    )
    return jax.shard_map(
        functools.partial(shards, mesh.shape["row"], mesh.shape["col"]),
        mesh=mesh, in_specs=placed, out_specs=P("row", "col"), check_vma=False,
    )
```

```python
import functools

import jax
import jax.numpy as jnp
from jax import lax
from jax.experimental import pallas as pl
from jax.experimental.pallas import tpu as pltpu
from jax.sharding import PartitionSpec as P

MESH = pl.DeviceIdType.MESH
F32 = jnp.float32
BF16 = jnp.bfloat16
LANES = 128
BLOCKS = 1


def others(at, count):
    if count & (count - 1):
        return [(step, lax.rem(at + step, count), count - step) for step in range(1, count)]
    out = []
    for step in range(1, count):
        to, weight = jnp.int32(0), 1
        while weight < count:
            bit = (at // weight) % 2
            to = to + weight * ((1 - bit) if step & weight else bit)
            weight *= 2
        out.append((step, to, step))
    return out


def split(x):
    high = x.astype(BF16)
    return high, (x - high.astype(F32)).astype(BF16)


def dot(a, b):
    return lax.dot_general(a, b, (((1,), (0,)), ((), ())), preferred_element_type=F32)


def dot_rt(a, b):
    return lax.dot_general(a, b, (((1,), (1,)), ((), ())), preferred_element_type=F32)


def pack(x, width):
    if width == 1:
        return x
    x = x.astype(F32)
    return jnp.stack([
        jnp.concatenate([x[p * width + w] for w in range(width)], axis=-1)
        for p in range(x.shape[0] // width)
    ]).astype(BF16)


def panel_kernel(
    n_row, n_col, order, rank,
    cu_hbm, cv_hbm, ru_hbm, rv_hbm, dl_hbm, du_hbm, trail_hbm,
    d_ref, gvall, trail,
    own, diag, mh, ml, cuall, cvall, guall,
    in_sem, cu_send, cu_recv, cv_send, cv_recv, gu_send, gu_recv, gv_send, gv_recv,
    row_hello, col_hello,
):
    row = lax.axis_index("row")
    col = lax.axis_index("col")
    paired = n_row % 2 == 0
    width = 2 if paired else 1
    chips = n_row // width
    core = row % width
    chip = row // width
    mate = chip * width + (1 - core) if paired else row
    nt, pieces = own.shape[1], guall.shape[1]
    wide = nt // pieces

    near = [(step, to * width + core, back) for step, to, back in others(chip, chips)]
    near_cols = others(col, n_col)
    row_peers = ([(0, mate, 0)] if paired else []) + near

    def load(src, dst, sem):
        copy = pltpu.make_async_copy(src, dst, sem)
        copy.start()
        return copy

    load(ru_hbm, own.at[0], in_sem.at[0])
    load(rv_hbm, own.at[1], in_sem.at[0])
    cv_load = load(cv_hbm, cvall.at[col], in_sem.at[3])
    cu_load = load(cu_hbm, cuall.at[col], in_sem.at[4])

    barrier = pltpu.get_barrier_semaphore()
    for _, to, _ in row_peers:
        @pl.when(to > row)
        def _():
            pl.semaphore_signal(barrier, inc=1, device_id=(to, col), device_id_type=MESH)
    for _, to, _ in near_cols:
        @pl.when(to > col)
        def _():
            pl.semaphore_signal(barrier, inc=1, device_id=(row, to), device_id_type=MESH)

    load(dl_hbm, diag.at[0], in_sem.at[1])
    load(du_hbm, diag.at[1], in_sem.at[1])
    trail_load = load(trail_hbm, trail, in_sem.at[2])

    lower_row = chip + (core if paired else 0)
    lower_col = col

    @pl.when(lower_row + lower_col > 0)
    def _():
        pl.semaphore_wait(barrier, lower_row + lower_col)

    def row_copy(buf, slot, send, recv, to):
        return pltpu.make_async_remote_copy(
            src_ref=buf.at[slot], dst_ref=buf.at[slot], send_sem=send, recv_sem=recv,
            device_id=(to, col), device_id_type=MESH,
        )

    def col_send(src, buf, send, recv, to):
        return pltpu.make_async_remote_copy(
            src_ref=src, dst_ref=buf.at[col], send_sem=send, recv_sem=recv,
            device_id=(row, to), device_id_type=MESH,
        )

    def cols_to(to, cv, cu):
        col_send(cv, cvall, cv_send, cv_recv, to).start()
        col_send(cu, cuall, cu_send, cu_recv, to).start()

    def rows_to(to, back):
        row_copy(guall, row, gu_send, gu_recv.at[back], to).start()
        row_copy(gvall, row, gv_send, gv_recv.at[back], to).start()

    for to in range(n_col):
        @pl.when(to < col)
        def _():
            cols_to(to, cv_hbm, cu_hbm)
    pltpu.make_async_copy(own, own, in_sem.at[0]).wait()
    guall[row] = pack(own[0], wide)
    gvall[row] = pack(own[1], wide)
    for _, to, back in reversed(row_peers):
        @pl.when(to < row)
        def _():
            rows_to(to, back)

    for _, to, back in row_peers:
        @pl.when(to < row)
        def _():
            pl.semaphore_signal(row_hello.at[back], inc=1, device_id=(to, col), device_id_type=MESH)
    for _, to, back in near_cols:
        @pl.when(to < col)
        def _():
            pl.semaphore_signal(col_hello.at[back], inc=1, device_id=(row, to), device_id_type=MESH)

    cv_load.wait()
    cu_load.wait()

    def greeted_row(step, to, back):
        @pl.when(to > row)
        def _():
            pl.semaphore_wait(row_hello.at[step], 1)
            rows_to(to, back)

    def greeted_col(step, to):
        @pl.when(to > col)
        def _():
            pl.semaphore_wait(col_hello.at[step], 1)
            cols_to(to, cvall.at[col], cuall.at[col])

    if paired:
        greeted_row(0, mate, 0)
    for n in range(max(len(near), len(near_cols))):
        if n == 0 and len(near) > 1:
            greeted_row(*near[0])
            greeted_row(*near[1])
        elif n > 0 and n + 1 < len(near):
            greeted_row(*near[n + 1])
        elif n == 0 and near:
            greeted_row(*near[0])
        if n < len(near_cols):
            greeted_col(*near_cols[n][:2])

    pltpu.make_async_copy(diag, diag, in_sem.at[1]).wait()
    half = order // 2
    uh, ul = split(diag[1])
    lh, ll = split(diag[0])

    def product(rows, mid, cols):
        a, b = uh[rows, mid], ul[rows, mid]
        c, d = lh[mid, cols], ll[mid, cols]
        return dot(a, c) + (dot(a, d) + dot(b, c))

    lo, hi, full = slice(0, half), slice(half, order), slice(0, order)
    for rows, mid, cols in ((lo, full, lo), (lo, hi, hi), (hi, hi, lo), (hi, hi, hi)):
        mh[rows, cols], ml[rows, cols] = split(product(rows, mid, cols))

    def arrive(buf, slot, send, recv, step):
        row_copy(buf, slot, send, recv.at[step], mate).wait_recv()
        if paired:
            row_copy(buf, slot, send, recv.at[0], mate).start()

    for step, slot, _ in near:
        arrive(guall, slot, gu_send, gu_recv, step)
    for step, slot, _ in near:
        arrive(gvall, slot, gv_send, gv_recv, step)

    def all_of(buf, count, send, recv):
        part = buf.at[pl.ds(0, count)]
        return pltpu.make_async_remote_copy(
            src_ref=part, dst_ref=part, send_sem=send, recv_sem=recv,
            device_id=(mate, col), device_id_type=MESH,
        )

    tiles = cvall.shape[1]
    trail_load.wait()
    if n_col > 1:
        all_of(cvall, n_col - 1, cv_send, cv_recv).wait_recv()
    weights = []
    for t in range(tiles):
        turned = jnp.concatenate([cvall[c, t] for c in range(n_col)], axis=-1)
        wh, wl = split(dot(turned, mh[...]) + dot(turned, ml[...]))
        weights.append(jnp.concatenate([wh, wl], axis=0))

    if n_col > 1:
        all_of(cuall, n_col - 1, cu_send, cu_recv).wait_recv()
    if paired:
        all_of(guall, chips, gu_send, gu_recv.at[0]).wait_recv()
    lanes = wide * rank
    spread = jnp.concatenate([guall[:, p].reshape(order, lanes) for p in range(pieces)], axis=-1)
    for t in range(tiles):
        turned = jnp.concatenate([cuall[c, t] for c in range(n_col)], axis=-1).astype(F32)
        left = jnp.concatenate([turned, turned], axis=0).T.astype(BF16)
        c = dot(weights[t], spread)
        ch, cl = split(c[:rank] + c[rank:])
        high = dot(left, jnp.concatenate([ch, cl], axis=0)).astype(BF16)
        for p in range(pieces):
            at = slice(p * lanes, (p + 1) * lanes)
            d_ref[t * pieces + p] = high[:, at]

    if paired:
        all_of(gvall, chips, gv_send, gv_recv.at[0]).wait_recv()
    if n_col > 1:
        all_of(cvall, n_col - 1, cv_send, cv_recv).wait_send()
        all_of(cuall, n_col - 1, cu_send, cu_recv).wait_send()
    if n_row > 1:
        all_of(guall, n_row - 1, gu_send, gu_recv.at[0]).wait_send()
        all_of(gvall, n_row - 1, gv_send, gv_recv.at[0]).wait_send()


def update_kernel(blocks, rank, d_ref, gv_ref, trail, out_hbm, out, out_sem):
    n_row, pieces, rc, lanes = gv_ref.shape
    order = n_row * rc
    count = order // blocks
    wide = lanes // rank
    tiles = d_ref.shape[0] // pieces
    for p in range(pieces):
        part = gv_ref[:, p].reshape(order, lanes)
        tile_of = lax.broadcasted_iota(jnp.int32, part.shape, 1) // rank
        for w in range(wide):
            only = jnp.where(tile_of == w, part.astype(F32), 0.0).astype(BF16) if wide > 1 else part
            right = only
            for b in range(blocks):
                for t in range(tiles):
                    rows = pl.ds(t * order, order)
                    at = pl.ds((p * wide + w) * order + b * count, count)
                    product = dot_rt(d_ref[t * pieces + p], right[b * count:(b + 1) * count])
                    out[rows, at] = (trail[rows, at].astype(F32) - product).astype(BF16)
                    pltpu.make_async_copy(out.at[rows, at], out_hbm.at[rows, at], out_sem).start()
    pltpu.make_async_copy(out, out_hbm, out_sem).wait()


def shards(n_row, n_col, trailing, col_u, col_v, row_u, row_v, diag_lower_inv, diag_upper_inv):
    mt, cc, rank = col_u.shape
    nt, rc, _ = row_u.shape
    order = diag_lower_inv.shape[0]
    anywhere = pl.BlockSpec(memory_space=pl.ANY)
    dma = pltpu.SemaphoreType.DMA
    vmem = pl.BlockSpec(memory_space=pltpu.VMEM)
    wide = max(1, LANES // rank)
    wide = wide if nt % wide == 0 else 1
    chips = n_row // 2 if n_row % 2 == 0 else n_row
    panel = pltpu.VMEM((n_row, nt // wide, rc, wide * rank), BF16)
    handed = pl.pallas_call(
        functools.partial(panel_kernel, n_row, n_col, order, rank),
        out_shape=[
            pltpu.VMEM((mt * nt // wide, order, wide * rank), BF16),
            panel,
            pltpu.VMEM(trailing.shape, BF16),
        ],
        in_specs=[anywhere] * 7,
        out_specs=[vmem] * 3,
        scratch_shapes=[
            pltpu.VMEM((2, *row_u.shape), BF16),
            pltpu.VMEM((2, order, order), F32),
            pltpu.VMEM((order, order), BF16),
            pltpu.VMEM((order, order), BF16),
            pltpu.VMEM((n_col, mt, rank, cc), BF16),
            pltpu.VMEM((n_col, mt, rank, cc), BF16),
            panel,
            dma((5,)), dma(()), dma(()), dma(()), dma(()),
            dma(()), dma((chips,)), dma(()), dma((chips,)),
            pltpu.SemaphoreType.REGULAR((chips,)), pltpu.SemaphoreType.REGULAR((n_col,)),
        ],
        compiler_params=pltpu.CompilerParams(collective_id=0, has_side_effects=True),
        name="panels",
    )(
        jnp.swapaxes(col_u, 1, 2), jnp.swapaxes(col_v, 1, 2), row_u, row_v,
        diag_lower_inv, diag_upper_inv, trailing,
    )
    handed = [pltpu.with_memory_space_constraint(x, pltpu.VMEM) for x in handed]
    return pl.pallas_call(
        functools.partial(update_kernel, BLOCKS, rank),
        out_shape=jax.ShapeDtypeStruct(trailing.shape, BF16),
        in_specs=[vmem] * 3,
        out_specs=anywhere,
        scratch_shapes=[pltpu.VMEM(trailing.shape, BF16), dma(())],
        name="update",
    )(*handed)


def solution(mesh):
    placed = (
        P("row", "col"),
        P("row", "col", None),
        P("row", "col", None),
        P("col", "row", None),
        P("col", "row", None),
        P(),
        P(),
    )
    return jax.shard_map(
        functools.partial(shards, mesh.shape["row"], mesh.shape["col"]),
        mesh=mesh, in_specs=placed, out_specs=P("row", "col"), check_vma=False,
    )
```

```python
import functools

import jax
import jax.numpy as jnp
from jax import lax
from jax.experimental import pallas as pl
from jax.experimental.pallas import tpu as pltpu
from jax.sharding import PartitionSpec as P

MESH = pl.DeviceIdType.MESH
F32 = jnp.float32
BF16 = jnp.bfloat16
LANES = 128
BLOCKS = 1


def others(at, count):
    if count & (count - 1):
        return [(step, lax.rem(at + step, count), count - step) for step in range(1, count)]
    out = []
    for step in range(1, count):
        to, weight = jnp.int32(0), 1
        while weight < count:
            bit = (at // weight) % 2
            to = to + weight * ((1 - bit) if step & weight else bit)
            weight *= 2
        out.append((step, to, step))
    return out


def split(x):
    high = x.astype(BF16)
    return high, (x - high.astype(F32)).astype(BF16)


def dot(a, b):
    return lax.dot_general(a, b, (((1,), (0,)), ((), ())), preferred_element_type=F32)


def dot_rt(a, b):
    return lax.dot_general(a, b, (((1,), (1,)), ((), ())), preferred_element_type=F32)


def pack(x, width):
    if width == 1:
        return x
    x = x.astype(F32)
    return jnp.stack([
        jnp.concatenate([x[p * width + w] for w in range(width)], axis=-1)
        for p in range(x.shape[0] // width)
    ]).astype(BF16)


def panel_kernel(
    n_row, n_col, order, rank,
    cu_hbm, cv_hbm, ru_hbm, rv_hbm, dl_hbm, du_hbm, trail_hbm,
    d_ref, gvall, trail,
    own, diag, mh, ml, cuall, cvall, guall,
    in_sem, cu_send, cu_recv, cv_send, cv_recv, gu_send, gu_recv, gv_send, gv_recv,
    row_hello, col_hello,
):
    row = lax.axis_index("row")
    col = lax.axis_index("col")
    paired = n_row % 2 == 0
    width = 2 if paired else 1
    chips = n_row // width
    core = row % width
    chip = row // width
    mate = chip * width + (1 - core) if paired else row
    nt, pieces = own.shape[1], guall.shape[1]
    wide = nt // pieces

    near = [(step, to * width + core, back) for step, to, back in others(chip, chips)]
    near_cols = others(col, n_col)
    row_peers = ([(0, mate, 0)] if paired else []) + near

    def load(src, dst, sem):
        copy = pltpu.make_async_copy(src, dst, sem)
        copy.start()
        return copy

    load(ru_hbm, own.at[0], in_sem.at[0])
    load(rv_hbm, own.at[1], in_sem.at[0])
    cv_load = load(cv_hbm, cvall.at[col], in_sem.at[3])
    cu_load = load(cu_hbm, cuall.at[col], in_sem.at[4])

    barrier = pltpu.get_barrier_semaphore()
    for _, to, _ in row_peers:
        @pl.when(to > row)
        def _():
            pl.semaphore_signal(barrier, inc=1, device_id=(to, col), device_id_type=MESH)
    for _, to, _ in near_cols:
        @pl.when(to > col)
        def _():
            pl.semaphore_signal(barrier, inc=1, device_id=(row, to), device_id_type=MESH)

    load(dl_hbm, diag.at[0], in_sem.at[1])
    load(du_hbm, diag.at[1], in_sem.at[1])
    trail_load = load(trail_hbm, trail, in_sem.at[2])

    lower_row = chip + (core if paired else 0)
    lower_col = col

    @pl.when(lower_row + lower_col > 0)
    def _():
        pl.semaphore_wait(barrier, lower_row + lower_col)

    def row_copy(buf, slot, send, recv, to):
        return pltpu.make_async_remote_copy(
            src_ref=buf.at[slot], dst_ref=buf.at[slot], send_sem=send, recv_sem=recv,
            device_id=(to, col), device_id_type=MESH,
        )

    def col_send(src, buf, send, recv, to):
        return pltpu.make_async_remote_copy(
            src_ref=src, dst_ref=buf.at[col], send_sem=send, recv_sem=recv,
            device_id=(row, to), device_id_type=MESH,
        )

    def cols_to(to, cv, cu):
        col_send(cv, cvall, cv_send, cv_recv, to).start()
        col_send(cu, cuall, cu_send, cu_recv, to).start()

    def rows_to(to, back):
        row_copy(guall, row, gu_send, gu_recv.at[back], to).start()
        row_copy(gvall, row, gv_send, gv_recv.at[back], to).start()

    for to in range(n_col):
        @pl.when(to < col)
        def _():
            cols_to(to, cv_hbm, cu_hbm)
    pltpu.make_async_copy(own, own, in_sem.at[0]).wait()
    guall[row] = pack(own[0], wide)
    gvall[row] = pack(own[1], wide)
    for _, to, back in reversed(row_peers):
        @pl.when(to < row)
        def _():
            rows_to(to, back)

    for _, to, back in row_peers:
        @pl.when(to < row)
        def _():
            pl.semaphore_signal(row_hello.at[back], inc=1, device_id=(to, col), device_id_type=MESH)
    for _, to, _ in near_cols:
        @pl.when(to < col)
        def _():
            pl.semaphore_signal(col_hello, inc=1, device_id=(row, to), device_id_type=MESH)

    cv_load.wait()
    cu_load.wait()

    def greeted_row(step, to, back):
        @pl.when(to > row)
        def _():
            pl.semaphore_wait(row_hello.at[step], 1)
            rows_to(to, back)

    if paired:
        greeted_row(0, mate, 0)
    for n in range(len(near)):
        if n == 0 and len(near) > 1:
            greeted_row(*near[0])
            greeted_row(*near[1])
        elif n > 0 and n + 1 < len(near):
            greeted_row(*near[n + 1])
        elif n == 0 and near:
            greeted_row(*near[0])

    higher_col = len(near_cols) - col

    @pl.when(higher_col > 0)
    def _():
        pl.semaphore_wait(col_hello, higher_col)
    for _, to, _ in near_cols:
        pl.when(to > col)(functools.partial(cols_to, to, cvall.at[col], cuall.at[col]))

    pltpu.make_async_copy(diag, diag, in_sem.at[1]).wait()
    half = order // 2
    uh, ul = split(diag[1])
    lh, ll = split(diag[0])

    def product(rows, mid, cols):
        a, b = uh[rows, mid], ul[rows, mid]
        c, d = lh[mid, cols], ll[mid, cols]
        return dot(a, c) + (dot(a, d) + dot(b, c))

    lo, hi, full = slice(0, half), slice(half, order), slice(0, order)
    for rows, mid, cols in ((lo, full, lo), (lo, hi, hi), (hi, hi, lo), (hi, hi, hi)):
        mh[rows, cols], ml[rows, cols] = split(product(rows, mid, cols))

    def arrive(buf, slot, send, recv, step):
        row_copy(buf, slot, send, recv.at[step], mate).wait_recv()
        if paired:
            row_copy(buf, slot, send, recv.at[0], mate).start()

    for step, slot, _ in near:
        arrive(guall, slot, gu_send, gu_recv, step)
    for step, slot, _ in near:
        arrive(gvall, slot, gv_send, gv_recv, step)

    def all_of(buf, count, send, recv):
        part = buf.at[pl.ds(0, count)]
        return pltpu.make_async_remote_copy(
            src_ref=part, dst_ref=part, send_sem=send, recv_sem=recv,
            device_id=(mate, col), device_id_type=MESH,
        )

    tiles = cvall.shape[1]
    trail_load.wait()
    if n_col > 1:
        all_of(cvall, n_col - 1, cv_send, cv_recv).wait_recv()
    weights = []
    for t in range(tiles):
        turned = jnp.concatenate([cvall[c, t] for c in range(n_col)], axis=-1)
        wh, wl = split(dot(turned, mh[...]) + dot(turned, ml[...]))
        weights.append(jnp.concatenate([wh, wl], axis=0))

    if n_col > 1:
        all_of(cuall, n_col - 1, cu_send, cu_recv).wait_recv()
    if paired:
        all_of(guall, chips, gu_send, gu_recv.at[0]).wait_recv()
    lanes = wide * rank
    spread = jnp.concatenate([guall[:, p].reshape(order, lanes) for p in range(pieces)], axis=-1)
    for t in range(tiles):
        turned = jnp.concatenate([cuall[c, t] for c in range(n_col)], axis=-1).astype(F32)
        left = jnp.concatenate([turned, turned], axis=0).T.astype(BF16)
        c = dot(weights[t], spread)
        ch, cl = split(c[:rank] + c[rank:])
        high = dot(left, jnp.concatenate([ch, cl], axis=0)).astype(BF16)
        for p in range(pieces):
            at = slice(p * lanes, (p + 1) * lanes)
            d_ref[t * pieces + p] = high[:, at]

    if paired:
        all_of(gvall, chips, gv_send, gv_recv.at[0]).wait_recv()
    if n_col > 1:
        all_of(cvall, n_col - 1, cv_send, cv_recv).wait_send()
        all_of(cuall, n_col - 1, cu_send, cu_recv).wait_send()
    if n_row > 1:
        all_of(guall, n_row - 1, gu_send, gu_recv.at[0]).wait_send()
        all_of(gvall, n_row - 1, gv_send, gv_recv.at[0]).wait_send()


def update_kernel(blocks, rank, d_ref, gv_ref, trail, out_hbm, out, out_sem):
    n_row, pieces, rc, lanes = gv_ref.shape
    order = n_row * rc
    count = order // blocks
    wide = lanes // rank
    tiles = d_ref.shape[0] // pieces
    for p in range(pieces):
        part = gv_ref[:, p].reshape(order, lanes)
        tile_of = lax.broadcasted_iota(jnp.int32, part.shape, 1) // rank
        for w in range(wide):
            only = jnp.where(tile_of == w, part.astype(F32), 0.0).astype(BF16) if wide > 1 else part
            right = only
            for b in range(blocks):
                for t in range(tiles):
                    rows = pl.ds(t * order, order)
                    at = pl.ds((p * wide + w) * order + b * count, count)
                    product = dot_rt(d_ref[t * pieces + p], right[b * count:(b + 1) * count])
                    out[rows, at] = (trail[rows, at].astype(F32) - product).astype(BF16)
                    pltpu.make_async_copy(out.at[rows, at], out_hbm.at[rows, at], out_sem).start()
    pltpu.make_async_copy(out, out_hbm, out_sem).wait()


def shards(n_row, n_col, trailing, col_u, col_v, row_u, row_v, diag_lower_inv, diag_upper_inv):
    mt, cc, rank = col_u.shape
    nt, rc, _ = row_u.shape
    order = diag_lower_inv.shape[0]
    anywhere = pl.BlockSpec(memory_space=pl.ANY)
    dma = pltpu.SemaphoreType.DMA
    vmem = pl.BlockSpec(memory_space=pltpu.VMEM)
    wide = max(1, LANES // rank)
    wide = wide if nt % wide == 0 else 1
    chips = n_row // 2 if n_row % 2 == 0 else n_row
    panel = pltpu.VMEM((n_row, nt // wide, rc, wide * rank), BF16)
    handed = pl.pallas_call(
        functools.partial(panel_kernel, n_row, n_col, order, rank),
        out_shape=[
            pltpu.VMEM((mt * nt // wide, order, wide * rank), BF16),
            panel,
            pltpu.VMEM(trailing.shape, BF16),
        ],
        in_specs=[anywhere] * 7,
        out_specs=[vmem] * 3,
        scratch_shapes=[
            pltpu.VMEM((2, *row_u.shape), BF16),
            pltpu.VMEM((2, order, order), F32),
            pltpu.VMEM((order, order), BF16),
            pltpu.VMEM((order, order), BF16),
            pltpu.VMEM((n_col, mt, rank, cc), BF16),
            pltpu.VMEM((n_col, mt, rank, cc), BF16),
            panel,
            dma((5,)), dma(()), dma(()), dma(()), dma(()),
            dma(()), dma((chips,)), dma(()), dma((chips,)),
            pltpu.SemaphoreType.REGULAR((chips,)), pltpu.SemaphoreType.REGULAR,
        ],
        compiler_params=pltpu.CompilerParams(collective_id=0, has_side_effects=True),
        name="panels",
    )(
        jnp.swapaxes(col_u, 1, 2), jnp.swapaxes(col_v, 1, 2), row_u, row_v,
        diag_lower_inv, diag_upper_inv, trailing,
    )
    handed = [pltpu.with_memory_space_constraint(x, pltpu.VMEM) for x in handed]
    return pl.pallas_call(
        functools.partial(update_kernel, BLOCKS, rank),
        out_shape=jax.ShapeDtypeStruct(trailing.shape, BF16),
        in_specs=[vmem] * 3,
        out_specs=anywhere,
        scratch_shapes=[pltpu.VMEM(trailing.shape, BF16), dma(())],
        name="update",
    )(*handed)


def solution(mesh):
    placed = (
        P("row", "col"),
        P("row", "col", None),
        P("row", "col", None),
        P("col", "row", None),
        P("col", "row", None),
        P(),
        P(),
    )
    return jax.shard_map(
        functools.partial(shards, mesh.shape["row"], mesh.shape["col"]),
        mesh=mesh, in_specs=placed, out_specs=P("row", "col"), check_vma=False,
    )
```
